32 devices in a mesh: gx: 4 (over y, x), gy: 8 (over z, core).
Axes of the slice: x: 2, y: 2, z: 4, core: 2. Of those that a mesh axis runs over, the one named last changes fastest.
Arguments:
- primal: float32 [4, 27, 16384], P(None, None, ('gx', 'gy')), may hold values from -6 to 6
- adjoint: float32 [4, 27, 16384], P(None, None, ('gx', 'gy')), may hold values from -6 to 6
- source: float32 [4, 27, 16384], P(None, None, ('gx', 'gy')), may hold values from -6 to 6
- coefficient: float32 [16384], P(('gx', 'gy')), may hold values from 0.3 to 3
- levels: int32 [16384], P(('gx', 'gy')), may hold values from 0 to 3
- recon: float32 [7, 125, 27], replicated, may hold values from -0.4375 to 0.4375
- stiffness: float32 [125, 27], replicated, may hold values from -1.25 to 1.25
- interp: float32 [125, 27], replicated, may hold values from -1.25 to 1.25
- flux: float32 [6, 25, 27], replicated, may hold values from -1.25 to 1.25
- face_eval: float32 [6, 25, 125], replicated, may hold values from -0.5 to 0.5
- child_interp: float32 [4, 25, 25], replicated, may hold values from -1.25 to 1.25
- ghost_send: int32 [32, 8, 32], P(('gx', 'gy')), may hold values from -1 to 511, as said below
- edge_send: int32 [32, 2, 16], P(('gx', 'gy')), may hold values from -1 to 511, as said below
- neighbor_slot: int32 [6, 16384], P(None, ('gx', 'gy')), may hold values from -1 to 799, as said below
- neighbor_child: int32 [6, 16384], P(None, ('gx', 'gy')), may hold values from 0 to 4, as said below
- hang_send: int32 [2, 32, 8, 8], P(None, ('gx', 'gy')), may hold values from -1 to 511, as said below
- hang_recv: int32 [3, 32, 8, 8], P(None, ('gx', 'gy')), may hold values from -1 to 511, as said below
Outputs:
- cell_indicator: float32 [4, 16384], P(None, ('gx', 'gy'))
- face_indicator: float32 [4, 16384], P(None, ('gx', 'gy'))
The draws below stay inside these ranges and needn't reach their ends.
Inputs may be any that keep to these rules, and one draw needn't show every extreme that they name: `ghost_send`: the gy index of a device numbers a block of a cube of blocks with side S, the cube root of 8: index = G(c0) + S * G(c1) + S * S * G(c2) for block coordinates c0, c1, c2, where G(p) = p xor (p // 2) is the Gray code, so face-adjacent blocks differ in one bit of the index. Row [r, p] lists the local cells that device r sends to the device with its gx index and gy index p, live ids first, then -1. Only the up to six blocks face-adjacent to r's block get live ids, between 16 and 32 of them, and exactly 32 go to the neighbour one step up along coordinate 0 wherever it exists. `edge_send`: row [r, 0] lists the local cells sent to the device one gx index lower with the same gy index, row [r, 1] those sent to the one higher, live ids first, then -1; where that device exists there are 8 to 16 live ids, and exactly 16 towards the lower one; otherwise the row is all -1. `neighbor_slot`: every slot that is not -1 points at a live entry: a cell of the device itself, a live entry of a gy peer's ghost_send row for this device, or a live entry of a gx neighbour's edge_send row towards this device. `neighbor_child`: 4 means a neighbour of the same level. `hang_send`: [0, r, p, t] is a local cell of device r and [1, r, p, t] one of its faces, both -1 after the live slots; live slots go only to face-adjacent gy peers (as for ghost_send), at most 8 to one peer, and the device with gy index 0 sends exactly 8 to each of its face-adjacent peers. `hang_recv`: [:, q, p, t] describes what device q receives in slot t from the device with its gx index and gy index p: a local coarse cell, its face (the opposite of the sender's fine face) and a child position 0 to 3; all three are -1 exactly where the sender's slot is empty.
All inputs are finite; a program needn't handle non-finite values.
Results may differ from the reference program's by a relative error of at most 0.0003.
Values sent between devices are 32-bit elements; how exact they have to be, the bound alone decides.
No kernel may reach another device: no remote copies, remote signals or barrier semaphores. Data moves between devices by JAX's collectives and lax.ppermute only.
A program may use at most 128 MiB of HBM per device.

```python
import math
import jax
import jax.numpy as jnp
from jax import lax

F = 4
DOFS = 27
QUADS = 125
FACEPTS = 25
CELL_DEV = 512
GSLOT = 32
XSLOT = 16
HSLOT = 8
CELLS = 16384
N_GY = 8
DEVICES = 32


def gray_encode(position):
    return jnp.bitwise_xor(position, position >> 1)


def gray_decode(code, side_log):
    position = code
    for shift_by in range(1, max(side_log, 1)):
        position = jnp.bitwise_xor(position, code >> shift_by)
    return position


def block_table():
    side_log = (N_GY.bit_length() - 1) // 3
    length = 1 << side_log
    own_rows = jnp.arange(N_GY, dtype=jnp.int32)
    coords = [gray_decode(own_rows >> side_log * axis_dim & length - 1, side_log) for axis_dim in range(3)]
    columns = []
    for axis_dim in range(3):
        for direction in (1, -1):
            moved = [coords[other] + (direction if other == axis_dim else 0) for other in range(3)]
            inside = (moved[axis_dim] >= 0) & (moved[axis_dim] < length)
            block_index = jnp.zeros((N_GY,), jnp.int32)
            for other in range(3):
                block_index = block_index + (gray_encode(moved[other] & length - 1) << side_log * other)
            columns.append(jnp.where(inside, block_index, -1))
    return jnp.stack(columns, 1)


def mesh_layout(key):
    segments = DEVICES // N_GY
    table = block_table()
    device = jnp.arange(DEVICES, dtype=jnp.int32)
    own_row = device % N_GY
    segment = device // N_GY
    peer_rows = jnp.arange(N_GY, dtype=jnp.int32)
    row_table = table[own_row]
    near = jnp.any(row_table[:, :, None] == peer_rows[None, None, :], axis=1)
    full = row_table[:, 0:1] == peer_rows[None, :]
    count = jax.random.randint(jax.random.fold_in(key, 11), (DEVICES, N_GY), GSLOT // 2, GSLOT + 1)
    count = jnp.where(full, GSLOT, count)
    count = jnp.where(near, count, 0)
    ghost_ids = jax.random.randint(jax.random.fold_in(key, 12), (DEVICES, N_GY, GSLOT), 0, CELL_DEV)
    ghost = jnp.where(jnp.arange(GSLOT)[None, None, :] < count[:, :, None], ghost_ids, -1)
    has_side = jnp.stack([segment > 0, segment < segments - 1], 1)
    edge_count = jax.random.randint(jax.random.fold_in(key, 13), (DEVICES, 2), XSLOT // 2, XSLOT + 1)
    edge_count = jnp.where(jnp.arange(2)[None, :] == 0, XSLOT, edge_count)
    edge_count = jnp.where(has_side, edge_count, 0)
    edge_ids = jax.random.randint(jax.random.fold_in(key, 14), (DEVICES, 2, XSLOT), 0, CELL_DEV)
    edge = jnp.where(jnp.arange(XSLOT)[None, None, :] < edge_count[:, :, None], edge_ids, -1)
    shape = (DEVICES, 6, CELL_DEV)
    kind_draw = jax.random.randint(jax.random.fold_in(key, 15), shape, 0, 20)
    local_cell = jax.random.randint(jax.random.fold_in(key, 16), shape, 0, CELL_DEV)
    direction = jax.random.randint(jax.random.fold_in(key, 17), shape, 0, 6)
    row_wide = jnp.broadcast_to(own_row[:, None, None], shape)
    first_peer = table[row_wide, direction]
    other_peer = table[row_wide, jnp.bitwise_xor(direction, 1)]
    source_row = jnp.where(first_peer >= 0, first_peer, other_peer)
    sender = segment[:, None, None] * N_GY + source_row
    live_count = jnp.maximum(count[sender, row_wide], 1)
    draw_bits = jax.random.randint(jax.random.fold_in(key, 18), shape, 0, 1 << 20)
    via_segment = CELL_DEV + source_row * GSLOT + draw_bits % live_count
    side_draw = jax.random.randint(jax.random.fold_in(key, 19), shape, 0, 2)
    low_ok = (segment > 0)[:, None, None]
    high_ok = (segment < segments - 1)[:, None, None]
    side_pick = jnp.where(side_draw == 0, jnp.where(low_ok, 0, 1), jnp.where(high_ok, 1, 0))
    side_ok = jnp.where(side_pick == 0, low_ok, high_ok)
    edge_sender = jnp.clip(device[:, None, None] + (2 * side_pick - 1) * N_GY, 0, DEVICES - 1)
    edge_live = jnp.maximum(edge_count[edge_sender, 1 - side_pick], 1)
    via_edges = CELL_DEV + N_GY * GSLOT + side_pick * XSLOT + draw_bits % edge_live
    chosen = jnp.where(kind_draw < 10, local_cell, jnp.where(kind_draw < 17, via_segment, jnp.where((kind_draw < 19) & side_ok, via_edges, -1)))
    neighbours = jnp.transpose(chosen, (1, 0, 2)).reshape(6, DEVICES * CELL_DEV)
    heavy = (jax.random.randint(jax.random.fold_in(key, 20), (DEVICES,), 0, 4) == 0) | (own_row == 0)
    light = jax.random.randint(jax.random.fold_in(key, 21), (DEVICES, N_GY), 0, HSLOT // 2 + 1)
    hang_count = jnp.where(heavy[:, None], HSLOT, light)
    hang_count = jnp.where(near, hang_count, 0)
    hang_live = jnp.arange(HSLOT)[None, None, :] < hang_count[:, :, None]
    hang_shape = (DEVICES, N_GY, HSLOT)
    fine_cell = jax.random.randint(jax.random.fold_in(key, 22), hang_shape, 0, CELL_DEV)
    fine_face = jax.random.randint(jax.random.fold_in(key, 23), hang_shape, 0, 6)
    coarse_cell = jax.random.randint(jax.random.fold_in(key, 24), hang_shape, 0, CELL_DEV)
    child_pos = jax.random.randint(jax.random.fold_in(key, 25), hang_shape, 0, 4)

    def turned(values):
        masked = jnp.where(hang_live, values, -1)
        return masked.reshape(segments, N_GY, N_GY, HSLOT).transpose(0, 2, 1, 3).reshape(DEVICES, N_GY, HSLOT)
    sent = jnp.stack([jnp.where(hang_live, fine_cell, -1), jnp.where(hang_live, fine_face, -1)])
    received = jnp.stack([turned(coarse_cell), turned(jnp.bitwise_xor(fine_face, 1)), turned(child_pos)])
    return (ghost, edge, neighbours, sent, received)


def draw_ghost_send(key, part):
    return mesh_layout(key)[0].astype(jnp.int32)


def draw_edge_send(key, part):
    return mesh_layout(key)[1].astype(jnp.int32)


def draw_neighbor_slot(key, part):
    return mesh_layout(key)[2].astype(jnp.int32)


def draw_hang_send(key, part):
    return mesh_layout(key)[3].astype(jnp.int32)


def draw_hang_recv(key, part):
    return mesh_layout(key)[4].astype(jnp.int32)


def draw_neighbor_child(key, part):
    child_draw = jax.random.randint(jax.random.fold_in(key, 31), (6, CELLS), 0, 20)
    return jnp.where(child_draw < 16, 4, child_draw - 16).astype(jnp.int32)


def touch_ends(entries, stream_key, least, top_value):
    spot = [jax.random.randint(jax.random.fold_in(stream_key, axis), (), 0, length) for axis, length in enumerate(entries.shape)]
    longest = entries.shape.index(max(entries.shape))
    beside = spot[:longest] + [(spot[longest] + 1) % entries.shape[longest]] + spot[longest + 1:]
    return entries.at[tuple(spot)].set(least).at[tuple(beside)].set(top_value)


def block_levels(key, dims, shards, smallest, high):
    def one(dim, parts):
        heights = jax.random.uniform(jax.random.fold_in(jax.random.fold_in(key, 6), dim), (parts,), jnp.float32, smallest / len(shards), high / len(shards))
        return jnp.repeat(jnp.exp(heights), dims[dim] // parts).reshape((-1,) + (1,) * (len(dims) - dim - 1))

    gain = one(*shards[0])
    for cut in shards[1:]:
        gain = gain * one(*cut)
    return gain


def noise(own_key, dims, spread, limit, split=(), kind=jnp.bfloat16):
    values = spread * jax.random.normal(own_key, dims, jnp.float32)
    if split:
        values = values * block_levels(own_key, dims, split, -0.22, 0.18)
    return jnp.clip(values, -limit, limit).astype(kind)


def setup_inputs(seed: int = 0) -> dict:
    arg_keys = jax.random.split(jax.random.key(seed), 18)
    primal = noise(arg_keys[0], (F, DOFS, CELLS), 1.0, 6.0, ((2, 32),), jnp.float32)
    adjoint = noise(arg_keys[1], (F, DOFS, CELLS), 1.0, 6.0, ((2, 32),), jnp.float32)
    source = noise(arg_keys[2], (F, DOFS, CELLS), 1.0, 6.0, ((2, 32),), jnp.float32)
    coefficient = jnp.clip(jnp.exp(math.log(3.0) - 2.3025851 * jax.random.uniform(arg_keys[3], (CELLS,), jnp.float32) ** block_levels(arg_keys[3], (CELLS,), ((0, 32),), -0.2, 0.2)), 0.3, 3.0)
    levels = touch_ends(jax.random.randint(arg_keys[4], (CELLS,), 0, 4), jax.random.fold_in(arg_keys[4], 1), 0, 3).astype(jnp.int32)
    recon = noise(arg_keys[5], (7, QUADS, DOFS), (7 * DOFS) ** -0.5, 0.4375, (), jnp.float32)
    stiffness = noise(arg_keys[6], (QUADS, DOFS), DOFS ** -0.5, 1.25, (), jnp.float32)
    interp = noise(arg_keys[7], (QUADS, DOFS), DOFS ** -0.5, 1.25, (), jnp.float32)
    flux = noise(arg_keys[8], (6, FACEPTS, DOFS), DOFS ** -0.5, 1.25, (), jnp.float32)
    face_eval = noise(arg_keys[9], (6, FACEPTS, QUADS), QUADS ** -0.5, 0.5, (), jnp.float32)
    child_interp = noise(arg_keys[10], (4, FACEPTS, FACEPTS), FACEPTS ** -0.5, 1.25, (), jnp.float32)
    ghost_send = draw_ghost_send(jax.random.fold_in(arg_keys[17], 71), 0)
    edge_send = draw_edge_send(jax.random.fold_in(arg_keys[17], 71), 0)
    neighbor_slot = draw_neighbor_slot(jax.random.fold_in(arg_keys[17], 71), 0)
    neighbor_child = draw_neighbor_child(jax.random.fold_in(arg_keys[17], 71), 0)
    hang_send = draw_hang_send(jax.random.fold_in(arg_keys[17], 71), 0)
    hang_recv = draw_hang_recv(jax.random.fold_in(arg_keys[17], 71), 0)
    return dict(primal=primal, adjoint=adjoint, source=source, coefficient=coefficient, levels=levels, recon=recon, stiffness=stiffness, interp=interp, flux=flux, face_eval=face_eval, child_interp=child_interp, ghost_send=ghost_send, edge_send=edge_send, neighbor_slot=neighbor_slot, neighbor_child=neighbor_child, hang_send=hang_send, hang_recv=hang_recv)


PRECISE = lax.Precision.HIGHEST
OPPOSITE = (1, 0, 3, 2, 5, 4)

def collect(blocks, cell_ids):
    safe_cells = jnp.maximum(cell_ids, 0)
    taken = jnp.take(blocks, safe_cells.reshape(-1), axis=2)
    taken = taken.reshape(blocks.shape[:2] + cell_ids.shape)
    return jnp.where(cell_ids >= 0, taken, 0.0)

def face_traces(flux, primal, cell_ids, face_ids):
    fine_u = collect(primal, cell_ids)
    flat_u = fine_u.reshape(fine_u.shape[0], fine_u.shape[1], -1)
    flat_faces = face_ids.reshape(-1)
    chosen = jnp.zeros((flat_u.shape[0], flux.shape[1], flat_u.shape[2]), jnp.float32)
    for face_idx in range(6):
        term = jnp.einsum('pj,kjs->kps', flux[face_idx], flat_u, precision=PRECISE)
        chosen = chosen + jnp.where(flat_faces == face_idx, term, 0.0)
    return chosen.reshape(chosen.shape[:2] + cell_ids.shape)

def take_back(face_total, traces_in, recv_maps, face_weight, child_interp):
    flat_trace = traces_in.reshape(traces_in.shape[0], traces_in.shape[1], -1)
    coarse = recv_maps[0].reshape(-1)
    coarse_face = recv_maps[1].reshape(-1)
    child_pos = recv_maps[2].reshape(-1)
    lifted = jnp.zeros_like(flat_trace)
    for position in range(4):
        term = jnp.einsum('qp,kqs->kps', child_interp[position], flat_trace, precision=PRECISE)
        lifted = lifted + jnp.where(child_pos == position, term, 0.0)
    target = jnp.maximum(coarse, 0)
    chosen = jnp.zeros_like(flat_trace)
    for face_idx in range(6):
        chosen = chosen + jnp.where(coarse_face == face_idx, jnp.take(face_weight[face_idx], target, axis=2), 0.0)
    contrib = jnp.where(coarse >= 0, lax.optimization_barrier(jnp.sum(lifted * chosen, axis=1)), 0.0)
    return face_total.at[:, target].add(contrib)

def local_terms(primal, adjoint, source, coefficient, recon, stiffness, interp, flux, face_eval, child_interp, primal_near, adjoint_near, buffer_slots, neighbor_child):
    is_live = buffer_slots >= 0
    safe_cells = jnp.maximum(buffer_slots, 0)
    weight = jnp.einsum('qj,kjc->kqc', recon[0], adjoint, precision=PRECISE)
    for face_idx in range(6):
        near_z = jnp.where(is_live[face_idx], jnp.take(adjoint_near, safe_cells[face_idx], axis=2), 0.0)
        weight = weight + jnp.einsum('qj,kjc->kqc', recon[face_idx + 1], near_z, precision=PRECISE)
    residual_q = jnp.einsum('qj,kjc->kqc', interp, source, precision=PRECISE) - coefficient * jnp.einsum('qj,kjc->kqc', stiffness, primal, precision=PRECISE)
    cell_part = lax.optimization_barrier(jnp.sum(residual_q * weight, axis=1))
    face_weight = jnp.einsum('fpq,kqc->fkpc', face_eval, weight, precision=PRECISE)
    face_total = jnp.zeros(cell_part.shape, jnp.float32)
    for face_idx in range(6):
        near_u = jnp.where(is_live[face_idx], jnp.take(primal_near, safe_cells[face_idx], axis=2), 0.0)
        outer_trace = jnp.einsum('pj,kjc->kpc', flux[OPPOSITE[face_idx]], near_u, precision=PRECISE)
        child_here = neighbor_child[face_idx]
        mapped = jnp.where(child_here == 4, outer_trace, 0.0)
        for position in range(4):
            term = jnp.einsum('pq,kqc->kpc', child_interp[position], outer_trace, precision=PRECISE)
            mapped = mapped + jnp.where(child_here == position, term, 0.0)
        inner_trace = jnp.einsum('pj,kjc->kpc', flux[face_idx], primal, precision=PRECISE)
        face_total = face_total + lax.optimization_barrier(jnp.sum((inner_trace + mapped) * face_weight[face_idx], axis=1))
    return (cell_part, face_total, face_weight)

def finish(cell_part, face_total, levels, quad_count, point_count):
    cell_size = jnp.exp2(-levels.astype(jnp.float32))
    return (cell_size * cell_part / math.sqrt(quad_count), cell_size * face_total / math.sqrt(6 * point_count))

def reference(primal, adjoint, source, coefficient, levels, recon, stiffness, interp, flux, face_eval, child_interp, ghost_send, edge_send, neighbor_slot, neighbor_child, hang_send, hang_recv):
    fields = primal.shape[0]

    def device(device_id):
        own_row = device_id % N_GY
        segment = device_id // N_GY
        first_cell = (device_id * CELL_DEV).astype(jnp.int32)
        own_u = lax.dynamic_slice_in_dim(primal, first_cell, CELL_DEV, 2)
        own_z = lax.dynamic_slice_in_dim(adjoint, first_cell, CELL_DEV, 2)
        own_src = lax.dynamic_slice_in_dim(source, first_cell, CELL_DEV, 2)
        coeff_cells = lax.dynamic_slice_in_dim(coefficient, first_cell, CELL_DEV, 0)
        level_cells = lax.dynamic_slice_in_dim(levels, first_cell, CELL_DEV, 0)
        slot_rows = lax.dynamic_slice_in_dim(neighbor_slot, first_cell, CELL_DEV, 1)
        child_rows = lax.dynamic_slice_in_dim(neighbor_child, first_cell, CELL_DEV, 1)
        shifted = slot_rows - CELL_DEV
        source_peer = jnp.clip(shifted // GSLOT, 0, N_GY - 1)
        ghost_pos = jnp.clip(shifted - source_peer * GSLOT, 0, GSLOT - 1)
        sender = segment * N_GY + source_peer
        via_segment = sender * CELL_DEV + ghost_send[sender, own_row, ghost_pos]
        edge_rel = shifted - N_GY * GSLOT
        side_pick = jnp.clip(edge_rel // XSLOT, 0, 1)
        edge_pos = jnp.clip(edge_rel - side_pick * XSLOT, 0, XSLOT - 1)
        edge_sender = jnp.clip(device_id + (2 * side_pick - 1) * N_GY, 0, DEVICES - 1)
        via_edges = edge_sender * CELL_DEV + edge_send[edge_sender, 1 - side_pick, edge_pos]
        global_ids = jnp.where(slot_rows < 0, -1, jnp.where(slot_rows < CELL_DEV, first_cell + slot_rows, jnp.where(shifted < N_GY * GSLOT, via_segment, via_edges)))
        global_ids = global_ids.astype(jnp.int32)
        cell_part, face_total, face_weight = local_terms(own_u, own_z, own_src, coeff_cells, recon, stiffness, interp, flux, face_eval, child_interp, primal, adjoint, global_ids, child_rows)
        senders = segment * N_GY + jnp.arange(N_GY, dtype=jnp.int32)
        fine_cell = hang_send[0][senders, own_row]
        fine_face = hang_send[1][senders, own_row]
        fine_ids = jnp.where(fine_cell >= 0, senders[:, None] * CELL_DEV + fine_cell, -1).astype(jnp.int32)
        traces_in = face_traces(flux, primal, fine_ids, fine_face)
        recv_maps = hang_recv[:, device_id]
        face_total = take_back(face_total, traces_in, recv_maps, face_weight, child_interp)
        return finish(cell_part, face_total, level_cells, recon.shape[1], flux.shape[1])
    cell_parts, face_parts = lax.map(device, jnp.arange(DEVICES, dtype=jnp.int32))
    cell_indicator = jnp.transpose(cell_parts, (1, 0, 2)).reshape(fields, DEVICES * CELL_DEV)
    face_indicator = jnp.transpose(face_parts, (1, 0, 2)).reshape(fields, DEVICES * CELL_DEV)
    return (cell_indicator, face_indicator)
```

```python
import math

import jax
import jax.numpy as jnp
from jax import lax
from jax.experimental import pallas as pl
from jax.experimental.pallas import tpu as pltpu
from jax.sharding import PartitionSpec as P

F32 = jnp.float32
BF16 = jnp.bfloat16
FACES = 6
CHILDREN = 4
KINDS = CHILDREN + 1


def up(value, unit):
    return -(-value // unit) * unit


def dot(a, b):
    return lax.dot_general(a, b, (((1,), (0,)), ((), ())), preferred_element_type=F32)


def dot_nt(a, b):
    return lax.dot_general(a, b, (((1,), (1,)), ((), ())), preferred_element_type=F32)


def split(x):
    hi = x.astype(BF16)
    return hi, (x - hi.astype(F32)).astype(BF16)


def iota(shape, axis):
    return lax.broadcasted_iota(jnp.int32, shape, axis)


def column(row):
    n = row.shape[1]
    spread = jnp.broadcast_to(row.astype(F32), (n, n))
    eye = iota((n, n), 0) == iota((n, n), 1)
    return jnp.sum(jnp.where(eye, spread, 0.0), axis=1, keepdims=True).astype(jnp.int32)


def onehot(mask):
    return jnp.where(mask, 1.0, 0.0).astype(BF16)


def placed_at(rows, width, offsets):
    rel = iota((rows, width), 1) - iota((rows, width), 0)
    hit = rel == offsets[0]
    for offset in offsets[1:]:
        hit = hit | (rel == offset)
    return onehot(hit)


class Sizes:
    def __init__(self, primal, ghost_send, edge_send, hang_send, recon, flux, peers):
        self.k, self.d, self.c = primal.shape
        self.dp = up(self.d, 32)
        self.rows = self.k * self.dp
        self.gs = ghost_send.shape[2]
        self.xs = edge_send.shape[2]
        self.hs = hang_send.shape[3]
        self.peers = peers
        self.bits = peers.bit_length() - 1
        self.msg = self.gs + self.hs
        self.remote = up(self.bits * self.gs + 2 * self.xs, 128)
        self.hp = 32
        while self.hp < self.bits * self.hs:
            self.hp *= 2
        self.hl = up(self.k * self.hp, 128)
        self.q = recon.shape[1]
        self.qp = up(self.q, 128)
        self.p = flux.shape[1]
        self.pp = up(self.p, 32)


def pack_kernel(n, primal, adjoint, ghost, edge, hang, *refs):
    outs, (data, picks) = refs[: n.bits + 2], refs[n.bits + 2 :]
    own = lax.axis_index("gy")
    data[...] = jnp.zeros(data.shape, F32)
    for k in range(n.k):
        data[k * n.dp : k * n.dp + n.d, :] = primal[k]
        data[n.rows + k * n.dp : n.rows + k * n.dp + n.d, :] = adjoint[k]
    for b in range(n.bits):
        partner = own ^ (1 << b)
        g = column(ghost[0, pl.ds(partner, 1), :])
        h = column(hang[0, 0, pl.ds(partner, 1), :])
        picks[b * n.msg : b * n.msg + n.gs, :] = jnp.where(g == iota((n.gs, n.c), 1), 1.0, 0.0)
        picks[b * n.msg + n.gs : (b + 1) * n.msg, :] = jnp.where(h == iota((n.hs, n.c), 1), 1.0, 0.0)
    base = n.bits * n.msg
    for side in range(2):
        e = column(edge[0, side : side + 1, :])
        picks[base + side * n.xs : base + (side + 1) * n.xs, :] = jnp.where(e == iota((n.xs, n.c), 1), 1.0, 0.0)
    hi, lo = split(data[...])
    sel = picks[...].astype(BF16)
    got = dot_nt(sel, hi) + dot_nt(sel, lo)
    for b in range(n.bits):
        outs[b][...] = got[b * n.msg : (b + 1) * n.msg]
    for side in range(2):
        outs[n.bits + side][...] = got[base + side * n.xs : base + (side + 1) * n.xs]


def local_kernel(
    n, primal, adjoint, source, coefficient, slots, hang_recv, recon, stiffness, interp, flux, face_eval, child,
    gathered, own2, residual, rw, mw, hw, fe, hcol, hrow, data, stack, faces, weights,
):
    own = lax.axis_index("gy")
    data[...] = jnp.zeros(data.shape, F32)
    for k in range(n.k):
        data[k * n.dp : k * n.dp + n.d, :] = primal[k]
        data[n.rows + k * n.dp : n.rows + k * n.dp + n.d, :] = adjoint[k]
    hi, lo = split(data[...])
    both = jnp.concatenate([hi, lo], axis=0)
    own2[...] = both
    for f in range(FACES):
        pick = onehot(slots[f : f + 1, :] == iota((n.c, n.c), 0))
        gathered[f] = dot(both, pick).astype(BF16)
    i_hi, i_lo = split(interp[...])
    s_hi, s_lo = split(stiffness[...])
    coeff = coefficient[...]
    for k in range(n.k):
        src_hi, src_lo = split(source[k])
        u_hi, u_lo = split(primal[k] * coeff)
        res = dot(i_hi, src_hi) + dot(i_hi, src_lo) + dot(i_lo, src_hi)
        res = res - (dot(s_hi, u_hi) + dot(s_hi, u_lo) + dot(s_lo, u_hi))
        residual[k, : n.q, :] = res
        if n.qp > n.q:
            residual[k, n.q :, :] = jnp.zeros((n.qp - n.q, n.c), F32)
    width = rw.shape[1]
    acc_hi = jnp.zeros((n.q, width), F32)
    acc_lo = jnp.zeros((n.q, width), F32)
    for m in range(1 + FACES):
        w_hi, w_lo = split(recon[m])
        acc_hi += dot(w_hi, placed_at(n.d, width, (2 * m * n.dp, (2 * m + 1) * n.dp)))
        acc_lo += dot(w_lo, placed_at(n.d, width, (2 * m * n.dp,)))
    weights[...] = jnp.zeros(weights.shape, F32)
    weights[: n.q, :] = acc_hi
    weights[n.qp : n.qp + n.q, :] = acc_lo
    rw[...] = weights[...].astype(BF16)
    stack[...] = jnp.zeros(stack.shape, F32)
    for h in range(CHILDREN):
        stack[0, h * n.pp : h * n.pp + n.p, : n.p] = child[h]
        stack[3, h * n.pp : h * n.pp + n.p, : n.p] = child[h].T
    width = mw.shape[2]
    for f in range(FACES):
        child_rows = stack[0, : CHILDREN * n.pp, : n.p]
        stack[1, : CHILDREN * n.pp, : n.d] = lax.dot_general(
            child_rows, flux[f ^ 1], (((1,), (0,)), ((), ())),
            precision=lax.Precision.HIGHEST, preferred_element_type=F32,
        )
        stack[1, CHILDREN * n.pp : CHILDREN * n.pp + n.p, : n.d] = flux[f ^ 1]
        for h in range(KINDS):
            stack[2, h * n.pp : h * n.pp + n.p, : n.d] = flux[f]
        m_hi, m_lo = split(stack[1, :, : n.d])
        f_hi, f_lo = split(stack[2, :, : n.d])
        mw[f] = (
            dot(m_hi, placed_at(n.d, width, (0, n.dp)))
            + dot(m_lo, placed_at(n.d, width, (2 * n.dp,)))
            + dot(f_hi, placed_at(n.d, width, (3 * n.dp, 4 * n.dp)))
            + dot(f_lo, placed_at(n.d, width, (5 * n.dp,)))
        ).astype(BF16)
        turned = lax.dot_general(
            stack[3, : CHILDREN * n.pp, : n.p], flux[f ^ 1], (((1,), (0,)), ((), ())),
            precision=lax.Precision.HIGHEST, preferred_element_type=F32,
        )
        t_hi, t_lo = split(turned)
        hw[f] = (
            dot(t_hi, placed_at(n.d, 3 * n.dp, (0, n.dp))) + dot(t_lo, placed_at(n.d, 3 * n.dp, (2 * n.dp,)))
        ).astype(BF16)
    faces[...] = jnp.zeros(faces.shape, F32)
    for f in range(FACES):
        faces[f * n.pp : f * n.pp + n.p, : n.q] = face_eval[f]
    e_hi, e_lo = split(faces[...])
    rows = FACES * n.pp
    fe[:rows, : n.qp] = e_hi
    fe[:rows, n.qp :] = e_hi
    fe[rows:, : n.qp] = e_lo
    fe[rows:, n.qp :] = jnp.zeros((rows, n.qp), BF16)
    hcol[...] = jnp.full(hcol.shape, -1.0, F32)
    for which in range(3):
        for b in range(n.bits):
            partner = own ^ (1 << b)
            col = column(hang_recv[which, 0, pl.ds(partner, 1), :]).astype(F32)
            for k in range(n.k):
                at = k * n.hp + b * n.hs
                hcol[at : at + n.hs, which * 128 : (which + 1) * 128] = jnp.broadcast_to(col, (n.hs, 128))
    eye = iota((n.hl, n.hl), 0) == iota((n.hl, n.hl), 1)
    for which in range(3):
        spread = jnp.broadcast_to(hcol[:, which * 128 : which * 128 + 1], (n.hl, n.hl))
        hrow[which : which + 1, :] = jnp.sum(jnp.where(eye, spread, 0.0), axis=0, keepdims=True)


def final_kernel(n, gathered, own2, residual, rw, mw, hw, fe, hcol, hrow, slots, kinds, levels, *refs):
    msgs = refs[: n.bits + 2]
    cell_out, face_out, incoming, hanging, zbuf, totals = refs[n.bits + 2 :]
    own = lax.axis_index("gy")
    incoming[...] = jnp.zeros(incoming.shape, F32)
    hanging[...] = jnp.zeros(hanging.shape, F32)
    for b in range(n.bits):
        incoming[b * n.gs : (b + 1) * n.gs, :] = msgs[b][: n.gs, :]
        hanging[b * n.hs : (b + 1) * n.hs, :] = msgs[b][n.gs :, : n.rows]
    base = n.bits * n.gs
    for side in range(2):
        incoming[base + side * n.xs : base + (side + 1) * n.xs, :] = msgs[n.bits + side][...]
    r_hi, r_lo = split(incoming[...].T)
    remote = jnp.concatenate([r_hi, r_lo], axis=0)
    place = iota((n.remote, n.c), 0)
    code = n.c + n.peers * n.gs + place - base
    for b in range(n.bits):
        inside = (place >= b * n.gs) & (place < (b + 1) * n.gs)
        code = jnp.where(inside, n.c + (own ^ (1 << b)) * n.gs + place - b * n.gs, code)
    code = jnp.where(place < base + 2 * n.xs, code, -2)
    hang_t = hanging[...].T
    if n.hl > hang_t.shape[1]:
        hang_t = jnp.concatenate([hang_t, jnp.zeros((n.rows, n.hl - hang_t.shape[1]), F32)], axis=1)
    spread = hang_t[: n.dp]
    for k in range(1, n.k):
        spread = spread + pltpu.roll(hang_t[k * n.dp : (k + 1) * n.dp], k * n.hp, 1)
    h_hi, h_lo = split(spread)
    h_in = jnp.concatenate([h_hi, h_lo, h_hi], axis=0)
    lifted = jnp.zeros((n.pp, n.hl), F32)
    for f in range(FACES):
        term = dot(hw[f], h_in)
        for h in range(CHILDREN):
            hit = (hrow[1:2, :] == f) & (hrow[2:3, :] == h)
            lifted = lifted + jnp.where(hit, term[h * n.pp : (h + 1) * n.pp], 0.0)
    lane = iota((n.pp, n.hl), 1)
    blocks = [
        jnp.where((lane >= k * n.hp) & (lane < (k + 1) * n.hp), lifted, 0.0) for k in range(n.k)
    ]
    l_hi, l_lo = split(jnp.concatenate(blocks, axis=0))
    target = (hcol[:, :1] + hcol[:, 128:129] * n.c).astype(jnp.int32)
    half = 2 * n.rows
    for k in range(n.k):
        for part in range(2):
            at = part * half + n.rows + k * n.dp
            zbuf[k, part * n.dp : (part + 1) * n.dp, :] = own2[at : at + n.dp, :]
    for f in range(FACES):
        got = gathered[f].astype(F32) + dot(remote, onehot(slots[f : f + 1, :] == code))
        got = got.astype(BF16)
        back = onehot(target - f * n.c == iota((n.hl, n.c), 1))
        extra = dot(l_hi, back) + dot(l_lo, back)
        kind = kinds[f : f + 1, :]
        for k in range(n.k):
            z_at = n.rows + k * n.dp
            for part in range(2):
                at = (2 * (1 + f) + part) * n.dp
                zbuf[k, at : at + n.dp, :] = got[part * half + z_at : part * half + z_at + n.dp]
            u_at = k * n.dp
            near_hi = got[u_at : u_at + n.dp]
            near_lo = got[half + u_at : half + u_at + n.dp]
            own_hi = own2[u_at : u_at + n.dp, :]
            own_lo = own2[half + u_at : half + u_at + n.dp, :]
            stacked = jnp.concatenate([near_hi, near_lo, near_hi, own_hi, own_lo, own_hi], axis=0)
            term = dot(mw[f], stacked)
            total = extra[k * n.pp : (k + 1) * n.pp]
            chosen = term[CHILDREN * n.pp :]
            for h in range(CHILDREN):
                chosen = jnp.where(kind == h, term[h * n.pp : (h + 1) * n.pp], chosen)
            totals[k, f * n.pp : (f + 1) * n.pp, :] = total + chosen
    size = jnp.exp2(-levels[...].astype(F32))
    rows = FACES * n.pp
    for k in range(n.k):
        both = dot(rw[...], zbuf[k])
        weight = both[: n.qp] + both[n.qp :]
        part = jnp.sum(residual[k] * weight, axis=0, keepdims=True)
        cell_out[k : k + 1, :] = size * part / math.sqrt(n.q)
        w_hi, w_lo = split(weight)
        both = dot(fe[...], jnp.concatenate([w_hi, w_lo], axis=0))
        face_weight = both[:rows] + both[rows:]
        part = jnp.sum(totals[k] * face_weight, axis=0, keepdims=True)
        face_out[k : k + 1, :] = size * part / math.sqrt(FACES * n.p)


def params():
    return pltpu.CompilerParams(vmem_limit_bytes=56 * 2**20)


def shards(
    primal, adjoint, source, coefficient, levels, recon, stiffness, interp, flux, face_eval, child_interp,
    ghost_send, edge_send, neighbor_slot, neighbor_child, hang_send, hang_recv,
):
    n = Sizes(primal, ghost_send, edge_send, hang_send, recon, flux, lax.axis_size("gy"))
    shape = jax.ShapeDtypeStruct
    lanes = 2 * n.rows
    sent = pl.pallas_call(
        lambda *refs: pack_kernel(n, *refs),
        out_shape=[shape((n.msg, lanes), F32)] * n.bits + [shape((n.xs, lanes), F32)] * 2,
        scratch_shapes=[
            pltpu.VMEM((lanes, n.c), F32),
            pltpu.VMEM((n.bits * n.msg + 2 * n.xs, n.c), F32),
        ],
        compiler_params=params(),
        name="pack",
    )(primal, adjoint, ghost_send, edge_send, hang_send)
    msgs = []
    for b in range(n.bits):
        pairs = [(i, i ^ (1 << b)) for i in range(n.peers)]
        msgs.append(lax.ppermute(sent[b], "gy", pairs))
    steps = lax.axis_size("gx")
    rising = [(i, i + 1) for i in range(steps - 1)]
    msgs.append(lax.ppermute(sent[n.bits + 1], "gx", rising))
    msgs.append(lax.ppermute(sent[n.bits], "gx", [(j, i) for i, j in rising]))
    local = pl.pallas_call(
        lambda *refs: local_kernel(n, *refs),
        out_shape=[
            shape((FACES, 2 * lanes, n.c), BF16),
            shape((2 * lanes, n.c), BF16),
            shape((n.k, n.qp, n.c), F32),
            shape((2 * n.qp, 2 * (1 + FACES) * n.dp), BF16),
            shape((FACES, KINDS * n.pp, 6 * n.dp), BF16),
            shape((FACES, CHILDREN * n.pp, 3 * n.dp), BF16),
            shape((2 * FACES * n.pp, 2 * n.qp), BF16),
            shape((n.hl, 3 * 128), F32),
            shape((8, n.hl), F32),
        ],
        scratch_shapes=[
            pltpu.VMEM((lanes, n.c), F32),
            pltpu.VMEM((4, KINDS * n.pp, 128), F32),
            pltpu.VMEM((FACES * n.pp, n.qp), F32),
            pltpu.VMEM((2 * n.qp, 2 * (1 + FACES) * n.dp), F32),
        ],
        compiler_params=params(),
        cost_estimate=pl.CostEstimate(flops=10**10, bytes_accessed=10**7, transcendentals=0),
        name="local",
    )(
        primal, adjoint, source, coefficient.reshape(1, n.c), neighbor_slot, hang_recv,
        recon, stiffness, interp, flux, face_eval, child_interp,
    )
    return tuple(
        pl.pallas_call(
            lambda *refs: final_kernel(n, *refs),
            out_shape=[shape((n.k, n.c), F32)] * 2,
            scratch_shapes=[
                pltpu.VMEM((n.remote, lanes), F32),
                pltpu.VMEM((up(n.bits * n.hs, 128), n.rows), F32),
                pltpu.VMEM((n.k, 2 * (1 + FACES) * n.dp, n.c), BF16),
                pltpu.VMEM((n.k, FACES * n.pp, n.c), F32),
            ],
            compiler_params=params(),
            name="finish",
        )(*local, neighbor_slot, neighbor_child, levels.reshape(1, n.c), *msgs)
    )


def solution(mesh):
    cells = ("gx", "gy")
    placed = (
        (P(None, None, cells),) * 3
        + (P(cells),) * 2
        + (P(),) * 6
        + (P(cells, None, None),) * 2
        + (P(None, cells),) * 2
        + (P(None, cells, None, None),) * 2
    )
    return jax.shard_map(
        shards,
        mesh=mesh,
        in_specs=placed,
        out_specs=(P(None, cells), P(None, cells)),
        check_vma=False,
    )
```

```python
import math

import jax
import jax.numpy as jnp
from jax import lax
from jax.experimental import pallas as pl
from jax.experimental.pallas import tpu as pltpu
from jax.sharding import PartitionSpec as P

F32 = jnp.float32
BF16 = jnp.bfloat16
FACES = 6
CHILDREN = 4
KINDS = CHILDREN + 1


def up(value, unit):
    return -(-value // unit) * unit


def dot(a, b):
    return lax.dot_general(a, b, (((1,), (0,)), ((), ())), preferred_element_type=F32)


def dot_nt(a, b):
    return lax.dot_general(a, b, (((1,), (1,)), ((), ())), preferred_element_type=F32)


def split(x):
    hi = x.astype(BF16)
    return hi, (x - hi.astype(F32)).astype(BF16)


def iota(shape, axis):
    return lax.broadcasted_iota(jnp.int32, shape, axis)


def column(row):
    n = row.shape[1]
    spread = jnp.broadcast_to(row.astype(F32), (n, n))
    eye = iota((n, n), 0) == iota((n, n), 1)
    return jnp.sum(jnp.where(eye, spread, 0.0), axis=1, keepdims=True).astype(jnp.int32)


def onehot(mask):
    return jnp.where(mask, 1.0, 0.0).astype(BF16)


def placed_at(rows, width, offsets):
    rel = iota((rows, width), 1) - iota((rows, width), 0)
    hit = rel == offsets[0]
    for offset in offsets[1:]:
        hit = hit | (rel == offset)
    return onehot(hit)


class Sizes:
    def __init__(self, primal, ghost_send, edge_send, hang_send, recon, flux, peers):
        self.k, self.d, self.c = primal.shape
        self.dp = up(self.d, 32)
        self.rows = self.k * self.dp
        self.gs = ghost_send.shape[2]
        self.xs = edge_send.shape[2]
        self.hs = hang_send.shape[3]
        self.peers = peers
        self.bits = peers.bit_length() - 1
        self.msg = self.gs + self.hs
        self.remote = up(self.bits * self.gs + 2 * self.xs, 128)
        self.hp = 32
        while self.hp < self.bits * self.hs:
            self.hp *= 2
        self.hl = up(self.k * self.hp, 128)
        self.q = recon.shape[1]
        self.qp = up(self.q, 128)
        self.p = flux.shape[1]
        self.pp = up(self.p, 32)


def pack_kernel(n, primal, adjoint, ghost, edge, hang, *refs):
    outs, (data, picks) = refs[: n.bits + 2], refs[n.bits + 2 :]
    own = lax.axis_index("gy")
    data[...] = jnp.zeros(data.shape, F32)
    for k in range(n.k):
        data[k * n.dp : k * n.dp + n.d, :] = primal[:, k, :]
        data[n.rows + k * n.dp : n.rows + k * n.dp + n.d, :] = adjoint[:, k, :]
    for b in range(n.bits):
        partner = own ^ (1 << b)
        g = column(ghost[0, pl.ds(partner, 1), :])
        h = column(hang[0, 0, pl.ds(partner, 1), :])
        picks[b * n.msg : b * n.msg + n.gs, :] = jnp.where(g == iota((n.gs, n.c), 1), 1.0, 0.0)
        picks[b * n.msg + n.gs : (b + 1) * n.msg, :] = jnp.where(h == iota((n.hs, n.c), 1), 1.0, 0.0)
    base = n.bits * n.msg
    for side in range(2):
        e = column(edge[0, side : side + 1, :])
        picks[base + side * n.xs : base + (side + 1) * n.xs, :] = jnp.where(e == iota((n.xs, n.c), 1), 1.0, 0.0)
    hi, lo = split(data[...])
    sel = picks[...].astype(BF16)
    got = dot_nt(sel, hi) + dot_nt(sel, lo)
    for b in range(n.bits):
        outs[b][...] = got[b * n.msg : (b + 1) * n.msg]
    for side in range(2):
        outs[n.bits + side][...] = got[base + side * n.xs : base + (side + 1) * n.xs]


def local_kernel(
    n, primal, adjoint, source, coefficient, slots, hang_recv, recon, stiffness, interp, flux, face_eval, child,
    gathered, own2, residual, rw, mw, hw, fe, hcol, hrow, data, stack, faces, weights,
):
    own = lax.axis_index("gy")
    data[...] = jnp.zeros(data.shape, F32)
    for k in range(n.k):
        data[k * n.dp : k * n.dp + n.d, :] = primal[:, k, :]
        data[n.rows + k * n.dp : n.rows + k * n.dp + n.d, :] = adjoint[:, k, :]
    hi, lo = split(data[...])
    both = jnp.concatenate([hi, lo], axis=0)
    own2[...] = both
    for f in range(FACES):
        pick = onehot(slots[f : f + 1, :] == iota((n.c, n.c), 0))
        gathered[f] = dot(both, pick).astype(BF16)
    i_hi, i_lo = split(interp[...].T)
    s_hi, s_lo = split(stiffness[...].T)
    coeff = coefficient[...]
    for k in range(n.k):
        src_hi, src_lo = split(source[:, k, :])
        u_hi, u_lo = split(primal[:, k, :] * coeff)
        res = dot(i_hi, src_hi) + dot(i_hi, src_lo) + dot(i_lo, src_hi)
        res = res - (dot(s_hi, u_hi) + dot(s_hi, u_lo) + dot(s_lo, u_hi))
        residual[k, : n.q, :] = res
        if n.qp > n.q:
            residual[k, n.q :, :] = jnp.zeros((n.qp - n.q, n.c), F32)
    width = rw.shape[1]
    acc_hi = jnp.zeros((n.q, width), F32)
    acc_lo = jnp.zeros((n.q, width), F32)
    for m in range(1 + FACES):
        w_hi, w_lo = split(recon[:, m, :].T)
        acc_hi += dot(w_hi, placed_at(n.d, width, (2 * m * n.dp, (2 * m + 1) * n.dp)))
        acc_lo += dot(w_lo, placed_at(n.d, width, (2 * m * n.dp,)))
    weights[...] = jnp.zeros(weights.shape, F32)
    weights[: n.q, :] = acc_hi
    weights[n.qp : n.qp + n.q, :] = acc_lo
    rw[...] = weights[...].astype(BF16)
    stack[...] = jnp.zeros(stack.shape, F32)
    for h in range(CHILDREN):
        stack[0, h * n.pp : h * n.pp + n.p, : n.p] = child[:, h, :]
        stack[3, h * n.pp : h * n.pp + n.p, : n.p] = child[:, h, :].T
    width = mw.shape[2]
    for f in range(FACES):
        child_rows = stack[0, : CHILDREN * n.pp, : n.p]
        stack[1, : CHILDREN * n.pp, : n.d] = lax.dot_general(
            child_rows, flux[f ^ 1], (((1,), (0,)), ((), ())),
            precision=lax.Precision.HIGHEST, preferred_element_type=F32,
        )
        stack[1, CHILDREN * n.pp : CHILDREN * n.pp + n.p, : n.d] = flux[f ^ 1]
        for h in range(KINDS):
            stack[2, h * n.pp : h * n.pp + n.p, : n.d] = flux[f]
        m_hi, m_lo = split(stack[1, :, : n.d])
        f_hi, f_lo = split(stack[2, :, : n.d])
        mw[f] = (
            dot(m_hi, placed_at(n.d, width, (0, n.dp)))
            + dot(m_lo, placed_at(n.d, width, (2 * n.dp,)))
            + dot(f_hi, placed_at(n.d, width, (3 * n.dp, 4 * n.dp)))
            + dot(f_lo, placed_at(n.d, width, (5 * n.dp,)))
        ).astype(BF16)
        turned = lax.dot_general(
            stack[3, : CHILDREN * n.pp, : n.p], flux[f ^ 1], (((1,), (0,)), ((), ())),
            precision=lax.Precision.HIGHEST, preferred_element_type=F32,
        )
        t_hi, t_lo = split(turned)
        hw[f] = (
            dot(t_hi, placed_at(n.d, 3 * n.dp, (0, n.dp))) + dot(t_lo, placed_at(n.d, 3 * n.dp, (2 * n.dp,)))
        ).astype(BF16)
    faces[...] = jnp.zeros(faces.shape, F32)
    for f in range(FACES):
        faces[f * n.pp : f * n.pp + n.p, : n.q] = face_eval[f]
    e_hi, e_lo = split(faces[...])
    rows = FACES * n.pp
    fe[:rows, : n.qp] = e_hi
    fe[:rows, n.qp :] = e_hi
    fe[rows:, : n.qp] = e_lo
    fe[rows:, n.qp :] = jnp.zeros((rows, n.qp), BF16)
    hcol[...] = jnp.full(hcol.shape, -1.0, F32)
    for which in range(3):
        for b in range(n.bits):
            partner = own ^ (1 << b)
            col = column(hang_recv[which, 0, pl.ds(partner, 1), :]).astype(F32)
            for k in range(n.k):
                at = k * n.hp + b * n.hs
                hcol[at : at + n.hs, which * 128 : (which + 1) * 128] = jnp.broadcast_to(col, (n.hs, 128))
    eye = iota((n.hl, n.hl), 0) == iota((n.hl, n.hl), 1)
    for which in range(3):
        spread = jnp.broadcast_to(hcol[:, which * 128 : which * 128 + 1], (n.hl, n.hl))
        hrow[which : which + 1, :] = jnp.sum(jnp.where(eye, spread, 0.0), axis=0, keepdims=True)


def final_kernel(n, gathered, own2, residual, rw, mw, hw, fe, hcol, hrow, slots, kinds, levels, *refs):
    msgs = refs[: n.bits + 2]
    cell_out, face_out, incoming, hanging, zbuf, totals = refs[n.bits + 2 :]
    own = lax.axis_index("gy")
    incoming[...] = jnp.zeros(incoming.shape, F32)
    hanging[...] = jnp.zeros(hanging.shape, F32)
    for b in range(n.bits):
        incoming[b * n.gs : (b + 1) * n.gs, :] = msgs[b][: n.gs, :]
        hanging[b * n.hs : (b + 1) * n.hs, :] = msgs[b][n.gs :, : n.rows]
    base = n.bits * n.gs
    for side in range(2):
        incoming[base + side * n.xs : base + (side + 1) * n.xs, :] = msgs[n.bits + side][...]
    r_hi, r_lo = split(incoming[...].T)
    remote = jnp.concatenate([r_hi, r_lo], axis=0)
    place = iota((n.remote, n.c), 0)
    code = n.c + n.peers * n.gs + place - base
    for b in range(n.bits):
        inside = (place >= b * n.gs) & (place < (b + 1) * n.gs)
        code = jnp.where(inside, n.c + (own ^ (1 << b)) * n.gs + place - b * n.gs, code)
    code = jnp.where(place < base + 2 * n.xs, code, -2)
    hang_t = hanging[...].T
    if n.hl > hang_t.shape[1]:
        hang_t = jnp.concatenate([hang_t, jnp.zeros((n.rows, n.hl - hang_t.shape[1]), F32)], axis=1)
    spread = hang_t[: n.dp]
    for k in range(1, n.k):
        spread = spread + pltpu.roll(hang_t[k * n.dp : (k + 1) * n.dp], k * n.hp, 1)
    h_hi, h_lo = split(spread)
    h_in = jnp.concatenate([h_hi, h_lo, h_hi], axis=0)
    lifted = jnp.zeros((n.pp, n.hl), F32)
    for f in range(FACES):
        term = dot(hw[f], h_in)
        for h in range(CHILDREN):
            hit = (hrow[1:2, :] == f) & (hrow[2:3, :] == h)
            lifted = lifted + jnp.where(hit, term[h * n.pp : (h + 1) * n.pp], 0.0)
    lane = iota((n.pp, n.hl), 1)
    blocks = [
        jnp.where((lane >= k * n.hp) & (lane < (k + 1) * n.hp), lifted, 0.0) for k in range(n.k)
    ]
    l_hi, l_lo = split(jnp.concatenate(blocks, axis=0))
    target = (hcol[:, :1] + hcol[:, 128:129] * n.c).astype(jnp.int32)
    half = 2 * n.rows
    for k in range(n.k):
        for part in range(2):
            at = part * half + n.rows + k * n.dp
            zbuf[k, part * n.dp : (part + 1) * n.dp, :] = own2[at : at + n.dp, :]
    for f in range(FACES):
        got = gathered[f].astype(F32) + dot(remote, onehot(slots[f : f + 1, :] == code))
        got = got.astype(BF16)
        back = onehot(target - f * n.c == iota((n.hl, n.c), 1))
        extra = dot(l_hi, back) + dot(l_lo, back)
        kind = kinds[f : f + 1, :]
        for k in range(n.k):
            z_at = n.rows + k * n.dp
            for part in range(2):
                at = (2 * (1 + f) + part) * n.dp
                zbuf[k, at : at + n.dp, :] = got[part * half + z_at : part * half + z_at + n.dp]
            u_at = k * n.dp
            near_hi = got[u_at : u_at + n.dp]
            near_lo = got[half + u_at : half + u_at + n.dp]
            own_hi = own2[u_at : u_at + n.dp, :]
            own_lo = own2[half + u_at : half + u_at + n.dp, :]
            stacked = jnp.concatenate([near_hi, near_lo, near_hi, own_hi, own_lo, own_hi], axis=0)
            term = dot(mw[f], stacked)
            total = extra[k * n.pp : (k + 1) * n.pp]
            chosen = term[CHILDREN * n.pp :]
            for h in range(CHILDREN):
                chosen = jnp.where(kind == h, term[h * n.pp : (h + 1) * n.pp], chosen)
            totals[k, f * n.pp : (f + 1) * n.pp, :] = total + chosen
    size = jnp.exp2(-levels[...].astype(F32))
    rows = FACES * n.pp
    for k in range(n.k):
        both = dot(rw[...], zbuf[k])
        weight = both[: n.qp] + both[n.qp :]
        part = jnp.sum(residual[k] * weight, axis=0, keepdims=True)
        cell_out[k : k + 1, :] = size * part / math.sqrt(n.q)
        w_hi, w_lo = split(weight)
        both = dot(fe[...], jnp.concatenate([w_hi, w_lo], axis=0))
        face_weight = both[:rows] + both[rows:]
        part = jnp.sum(totals[k] * face_weight, axis=0, keepdims=True)
        face_out[k : k + 1, :] = size * part / math.sqrt(FACES * n.p)


def params():
    return pltpu.CompilerParams(vmem_limit_bytes=56 * 2**20)


def shards(
    primal, adjoint, source, coefficient, levels, recon, stiffness, interp, flux, face_eval, child_interp,
    ghost_send, edge_send, neighbor_slot, neighbor_child, hang_send, hang_recv,
):
    n = Sizes(primal, ghost_send, edge_send, hang_send, recon, flux, lax.axis_size("gy"))
    shape = jax.ShapeDtypeStruct
    primal, adjoint, source, child_interp = (
        jnp.transpose(x, (1, 0, 2)) for x in (primal, adjoint, source, child_interp)
    )
    recon = jnp.transpose(recon, (2, 0, 1))
    lanes = 2 * n.rows
    sent = pl.pallas_call(
        lambda *refs: pack_kernel(n, *refs),
        out_shape=[shape((n.msg, lanes), F32)] * n.bits + [shape((n.xs, lanes), F32)] * 2,
        scratch_shapes=[
            pltpu.VMEM((lanes, n.c), F32),
            pltpu.VMEM((n.bits * n.msg + 2 * n.xs, n.c), F32),
        ],
        compiler_params=params(),
        name="pack",
    )(primal, adjoint, ghost_send, edge_send, hang_send)
    msgs = []
    for b in range(n.bits):
        pairs = [(i, i ^ (1 << b)) for i in range(n.peers)]
        msgs.append(lax.ppermute(sent[b], "gy", pairs))
    steps = lax.axis_size("gx")
    rising = [(i, i + 1) for i in range(steps - 1)]
    msgs.append(lax.ppermute(sent[n.bits + 1], "gx", rising))
    msgs.append(lax.ppermute(sent[n.bits], "gx", [(j, i) for i, j in rising]))
    local = pl.pallas_call(
        lambda *refs: local_kernel(n, *refs),
        out_shape=[
            shape((FACES, 2 * lanes, n.c), BF16),
            shape((2 * lanes, n.c), BF16),
            shape((n.k, n.qp, n.c), F32),
            shape((2 * n.qp, 2 * (1 + FACES) * n.dp), BF16),
            shape((FACES, KINDS * n.pp, 6 * n.dp), BF16),
            shape((FACES, CHILDREN * n.pp, 3 * n.dp), BF16),
            shape((2 * FACES * n.pp, 2 * n.qp), BF16),
            shape((n.hl, 3 * 128), F32),
            shape((8, n.hl), F32),
        ],
        scratch_shapes=[
            pltpu.VMEM((lanes, n.c), F32),
            pltpu.VMEM((4, KINDS * n.pp, 128), F32),
            pltpu.VMEM((FACES * n.pp, n.qp), F32),
            pltpu.VMEM((2 * n.qp, 2 * (1 + FACES) * n.dp), F32),
        ],
        compiler_params=params(),
        cost_estimate=pl.CostEstimate(flops=10**10, bytes_accessed=10**7, transcendentals=0),
        name="local",
    )(
        primal, adjoint, source, coefficient.reshape(1, n.c), neighbor_slot, hang_recv,
        recon, stiffness.T, interp.T, flux, face_eval, child_interp,
    )
    return tuple(
        pl.pallas_call(
            lambda *refs: final_kernel(n, *refs),
            out_shape=[shape((n.k, n.c), F32)] * 2,
            scratch_shapes=[
                pltpu.VMEM((n.remote, lanes), F32),
                pltpu.VMEM((up(n.bits * n.hs, 128), n.rows), F32),
                pltpu.VMEM((n.k, 2 * (1 + FACES) * n.dp, n.c), BF16),
                pltpu.VMEM((n.k, FACES * n.pp, n.c), F32),
            ],
            compiler_params=params(),
            name="finish",
        )(*local, neighbor_slot, neighbor_child, levels.reshape(1, n.c), *msgs)
    )


def solution(mesh):
    cells = ("gx", "gy")
    placed = (
        (P(None, None, cells),) * 3
        + (P(cells),) * 2
        + (P(),) * 6
        + (P(cells, None, None),) * 2
        + (P(None, cells),) * 2
        + (P(None, cells, None, None),) * 2
    )
    return jax.shard_map(
        shards,
        mesh=mesh,
        in_specs=placed,
        out_specs=(P(None, cells), P(None, cells)),
        check_vma=False,
    )
```
